8 devices in a mesh: model: 1 (over z), replica: 2 (over y), fsdp: 4 (over x, core).
Axes of the slice: x: 2, y: 2, z: 1, core: 2. Of those that a mesh axis runs over, the one named last changes fastest.
Arguments:
- x_in: bfloat16 [2, 16384, 1024], P(None, ('model', 'replica', 'fsdp'))
- dy_out: bfloat16 [2, 16384, 1024], P(None, ('model', 'replica', 'fsdp'))
- lengths: int32 [2, 8], P(None, ('model', 'replica', 'fsdp'))
- w_up: bfloat16 [4, 1024, 4096], P(None, ('model', 'fsdp'))
- w_down: bfloat16 [4, 4096, 1024], P(None, ('model', 'fsdp'))
Outputs:
- output 1: float32 [4, 1024, 4096], P(None, ('model', 'fsdp'))
- output 2: float32 [4, 4096, 1024], P(None, ('model', 'fsdp'))
All inputs are finite; a program needn't handle non-finite values.
Results may differ from the reference program's by a relative error of at most 0.00910575.
Values are sent between devices in bfloat16 or wider.
A program may use at most 1 GiB of HBM per device.

```python
import jax
import jax.numpy as jnp
from jax import lax

D_MODEL = 1024
D_FF = 4096
N_LAYERS = 4
N_MICRO = 2
TOK_DEV = 2048
N_REPLICA = 2
N_FSDP = 4

GROUP_DEV = N_REPLICA * N_FSDP
TOKENS = GROUP_DEV * TOK_DEV


def setup_inputs(seed: int = 0, part: int = 0) -> dict:
    base_key = jax.random.fold_in(jax.random.key(seed), part)
    key_list = jax.random.split(base_key, 5)
    grad_scale = (N_MICRO * TOKENS) ** -0.5
    x_in = jax.random.normal(key_list[0], (N_MICRO, TOKENS, D_MODEL), jnp.float32).astype(jnp.bfloat16)
    dy_out = (jax.random.normal(key_list[1], (N_MICRO, TOKENS, D_MODEL), jnp.float32) * grad_scale).astype(jnp.bfloat16)
    lengths = jax.random.randint(key_list[2], (N_MICRO, GROUP_DEV), TOK_DEV // 4, TOK_DEV + 1, dtype=jnp.int32)
    lengths = lengths.at[0, 0].set(TOK_DEV).at[N_MICRO - 1, GROUP_DEV - 1].set(TOK_DEV // 4)
    w_up = (jax.random.normal(key_list[3], (N_LAYERS, D_MODEL, D_FF), jnp.float32) * D_MODEL ** -0.5).astype(jnp.bfloat16)
    w_down = (jax.random.normal(key_list[4], (N_LAYERS, D_FF, D_MODEL), jnp.float32) * D_FF ** -0.5).astype(jnp.bfloat16)
    return {"x_in": x_in, "dy_out": dy_out, "lengths": lengths, "w_up": w_up, "w_down": w_down}


def layer_forward(x_cur, weights):
    w_up_l, w_down_l = weights
    hidden = jnp.dot(x_cur, w_up_l, preferred_element_type=jnp.float32).astype(jnp.bfloat16)
    act_bf = jax.nn.gelu(hidden.astype(jnp.float32)).astype(jnp.bfloat16)
    x_next = (x_cur.astype(jnp.float32) + jnp.dot(act_bf, w_down_l, preferred_element_type=jnp.float32)).astype(jnp.bfloat16)
    return x_next, (x_cur, hidden)


def layer_backward(grad_x, item):
    w_up_l, w_down_l, x_cur, hidden = item
    act_f32, gelu_vjp = jax.vjp(jax.nn.gelu, hidden.astype(jnp.float32))
    act_bf = act_f32.astype(jnp.bfloat16)
    grad_act = jnp.dot(grad_x, w_down_l.T, preferred_element_type=jnp.float32)
    grad_hid = gelu_vjp(grad_act)[0].astype(jnp.bfloat16)
    gw_down = jnp.dot(act_bf.T, grad_x, preferred_element_type=jnp.float32)
    gw_up = jnp.dot(x_cur.T, grad_hid, preferred_element_type=jnp.float32)
    grad_prev = (grad_x.astype(jnp.float32) + jnp.dot(grad_hid, w_up_l.T, preferred_element_type=jnp.float32)).astype(jnp.bfloat16)
    return grad_prev, (gw_up, gw_down)


def reference(x_in, dy_out, lengths, w_up, w_down):
    n_blocks = N_MICRO * GROUP_DEV
    x_blocks = x_in.reshape(n_blocks, TOK_DEV, D_MODEL)
    dy_blocks = dy_out.reshape(n_blocks, TOK_DEV, D_MODEL)
    len_blocks = lengths.reshape(n_blocks)

    def block_grads(acc_pair, block_in):
        x_blk, dy_blk, len_blk = block_in
        _, saved_acts = lax.scan(layer_forward, x_blk, (w_up, w_down))
        token_mask = jnp.arange(TOK_DEV) < len_blk
        grad_top = jnp.where(token_mask[:, None], dy_blk, jnp.zeros_like(dy_blk))
        _, grads = lax.scan(layer_backward, grad_top, (w_up, w_down, saved_acts[0], saved_acts[1]), reverse=True)
        return (acc_pair[0] + grads[0], acc_pair[1] + grads[1]), None

    init_pair = (jnp.zeros((N_LAYERS, D_MODEL, D_FF), jnp.float32), jnp.zeros((N_LAYERS, D_FF, D_MODEL), jnp.float32))
    (grad_up, grad_down), _ = lax.scan(block_grads, init_pair, (x_blocks, dy_blocks, len_blocks))
    return grad_up, grad_down
```

```python
import jax
import jax.numpy as jnp
from jax import lax
from jax.experimental import pallas as pl
from jax.experimental.pallas import tpu as pltpu
from jax.sharding import PartitionSpec as P


BF = jnp.bfloat16
F32 = jnp.float32
BLK = 32
TB = 512
NBUF = 3
K0 = 0.7978845608028654
K1 = 0.044715
TYP = 3584
SWAP_CORE = [(0, 1), (1, 0), (2, 3), (3, 2)]
SWAP_X = [(0, 2), (2, 0), (1, 3), (3, 1)]
WHOLE = (0, 3, 5, 6, 7)
CLASS_STEP = (1, 4, 5)
ANY = pl.BlockSpec(memory_space=pl.ANY)
NT = (((1,), (1,)), ((), ()))
TN = (((0,), (0,)), ((), ()))


def gelu_of(h):
    return h * (0.5 + 0.5 * jnp.tanh(h * (K0 + (K0 * K1) * (h * h))))


def gelu_grad_of(h):
    hh = h * h
    s = 0.5 + 0.5 * jnp.tanh(h * (K0 + (K0 * K1) * hh))
    return s + ((s * (1.0 - s)) * h) * ((2.0 * K0) + (6.0 * K0 * K1) * hh)


def load_weight(meta, layer, parts, w, sem, first=0):
    own, par, *far = parts
    x, c, y = meta[0], meta[1], meta[2]
    unit = own.shape[1]
    half = unit // 2
    o = 1 - x
    mine, other = (2 * o + c) * unit, (2 * o + 1 - c) * unit
    rows = [(own.at[layer], (2 * x + c) * unit, unit), (par.at[layer], (2 * x + 1 - c) * unit, unit)]
    if len(far) == 2:
        rows += [(far[0], mine, unit), (far[1], other, unit)]
    else:
        low, high = y * half, (1 - y) * half
        rows += [(far[0], mine + low, half), (far[1], mine + high, half)]
        rows += [(far[2], other + low, half), (far[3], other + high, half)]
    size = w.shape[0]

    def each(act):
        for k, (src, row, n) in enumerate(rows):
            if size == 4 * unit:
                at = pl.multiple_of(row, half)
                act(pltpu.make_async_copy(src, w.at[pl.ds(at, n)], sem.at[k]))
            else:
                @pl.when(row // size == first)
                def _(src=src, row=row, n=n, k=k):
                    at = pl.multiple_of(row - first * size, half)
                    act(pltpu.make_async_copy(src, w.at[pl.ds(at, n)], sem.at[k]))

    each(lambda cp: cp.start())
    each(lambda cp: cp.wait())


def tile(rows, cols, col=None):
    pick = col or (lambda m: 0)
    return pl.BlockSpec((rows, cols), lambda t, m: (jnp.minimum(t, m[5] - 1), pick(m)))


def call(body, grid, in_specs, out_specs, out_shape, args, deps, scratch, flops, nbytes, aliases=None):
    n_in, n_dep, n_out = len(args), len(deps), len(out_shape)

    def kern(meta, *refs):
        rest = refs[n_in + n_dep:]
        body(meta, refs[:n_in], rest[:n_out], rest[n_out + 1:])

    def run(meta):
        return pl.pallas_call(
            kern,
            grid_spec=pltpu.PrefetchScalarGridSpec(
                num_scalar_prefetch=1,
                grid=grid,
                in_specs=list(in_specs) + [ANY] * n_dep,
                out_specs=list(out_specs) + [ANY],
                scratch_shapes=scratch,
            ),
            out_shape=list(out_shape) + [jax.ShapeDtypeStruct((8, 128), F32)],
            input_output_aliases=aliases or {},
            cost_estimate=pl.CostEstimate(flops=flops, bytes_accessed=nbytes, transcendentals=0),
            compiler_params=pltpu.CompilerParams(
                dimension_semantics=("arbitrary",) * len(grid), vmem_limit_bytes=67043328
            ),
        )(meta, *args, *deps)

    return run


def live_tiles(meta, t, compute):
    @pl.when(t < meta[6])
    def _():
        compute(slice(0, TB))

    @pl.when((t >= meta[6]) & (t < meta[5]))
    def _():
        compute(slice(0, TB // 2))


def gradient_out(t, last_live, last, acc, dsts, sem):
    n = acc.shape[1] // len(dsts)
    copies = [
        pltpu.make_async_copy(acc.at[:, pl.ds(k * n, n)], dst, sem.at[k]) for k, dst in enumerate(dsts)
    ]

    @pl.when(t == last_live)
    def _():
        for cp in copies:
            cp.start()

    @pl.when(t == last)
    def _():
        for cp in copies:
            cp.wait()


def blocks_of(cls, n_blk):
    low = n_blk // 2
    first = [b for b in range(low) if b % 2 == cls]
    return first + [b for b in range(low, n_blk) if (b - low) % 4 == cls]


def count_of(length, cls, tok):
    low = jnp.minimum(length, tok // 2)
    high = length - low

    def share(n, ways):
        return (n // (ways * BLK)) * BLK + jnp.clip(n % (ways * BLK) - cls * BLK, 0, BLK)

    return (share(low, 2) if cls < 2 else 0) + share(high, 4)


def split(v, deps=()):
    n_micro, n_blk, blk, d = v.shape
    lists = [blocks_of(cls, n_blk) for cls in (1, 2, 3)]

    def body(meta, ins, outs, scr):
        bufs, isem, osem = scr[:3], scr[3], scr[4]
        takes = [
            [
                pltpu.make_async_copy(ins[0].at[k, b], buf.at[k, pl.ds(n * blk, blk)], isem.at[c])
                for k in range(n_micro) for n, b in enumerate(lists[c])
            ]
            for c, buf in enumerate(bufs)
        ]
        gives = [pltpu.make_async_copy(buf, o, osem.at[c]) for c, (buf, o) in enumerate(zip(bufs, outs))]
        order = (1, 2, 0)
        for c in order:
            for cp in takes[c]:
                cp.start()
        for c in order:
            for cp in takes[c]:
                cp.wait()
            gives[c].start()
        for cp in gives:
            cp.wait()

    shapes = [(n_micro, len(x) * blk, d) for x in lists]
    return call(
        body, (1,), [ANY], [ANY] * 3, [jax.ShapeDtypeStruct(s, BF) for s in shapes], (v,), deps,
        [pltpu.VMEM(s, BF) for s in shapes] + [pltpu.SemaphoreType.DMA((3,))] * 2,
        TYP * d * 1000, n_micro * n_blk * blk * d * 3,
    )(jnp.zeros((1,), jnp.int32))


def pack(meta, v, gots, masked, deps=()):
    n_micro, n_blk, blk, d = v.shape
    mine = blocks_of(0, n_blk)
    total = n_micro * n_blk * blk
    seqs = [(None, k) for k in range(n_micro)] + [(c, k) for c in range(len(gots)) for k in range(n_micro)]
    longest = len(mine) * blk

    def body(meta, ins, outs, scr):
        v_hbm, *got = ins
        (o_hbm,) = outs
        buf, zero, isem, osem = scr
        takes = []
        for s, (c, k) in enumerate(seqs):
            if c is None:
                takes.append([
                    pltpu.make_async_copy(v_hbm.at[k, b], buf.at[s, pl.ds(n * blk, blk)], isem.at[s])
                    for n, b in enumerate(mine)
                ])
            else:
                n = gots[c].shape[1]
                takes.append([pltpu.make_async_copy(got[c].at[k], buf.at[s, pl.ds(0, n)], isem.at[s])])
        for copies in takes:
            for cp in copies:
                cp.start()
        zero[...] = jnp.zeros_like(zero)

        def pieces(src, off, n, largest):
            at, out = jnp.int32(0), []
            size = largest
            while size >= 16:
                on = (n // size) % 2 == 1
                here = pl.ds(pl.multiple_of(at, 16), size) if src is not zero else pl.ds(0, size)
                there = pl.ds(pl.multiple_of(off + at, 16), size)
                out.append((on, pltpu.make_async_copy(src.at[here], o_hbm.at[there], osem)))
                at = at + jnp.where(on, size, 0)
                size //= 2
            return out

        gives, off = [], jnp.int32(0)
        for s in range(len(seqs)):
            n = meta[8 + s]
            for cp in takes[s]:
                cp.wait()
            if masked:
                base = n // 16 * 16

                @pl.when(n > base)
                def _(s=s, n=n, base=base):
                    row = pl.ds(pl.multiple_of(base, 16), 16)
                    at = lax.broadcasted_iota(jnp.int32, (16, d), 0) + base
                    buf[s, row, :] = jnp.where(at < n, buf[s, row, :].astype(F32), 0.0).astype(BF)

            n = (n + 15) // 16 * 16
            for on, cp in pieces(buf.at[s], off, n, 512):
                gives.append((on, cp))
                pl.when(on)(cp.start)
            off = off + n
        for on, cp in pieces(zero, off, meta[5] * TB - off, 256):
            gives.append((on, cp))
            pl.when(on)(cp.start)
        for on, cp in gives:
            pl.when(on)(cp.wait)

    return call(
        body, (1,), [ANY] * (1 + len(gots)), [ANY], [jax.ShapeDtypeStruct((total, d), BF)], (v,) + tuple(gots), deps,
        [pltpu.VMEM((len(seqs), longest, d), BF), pltpu.VMEM((TB // 2, d), BF), pltpu.SemaphoreType.DMA((len(seqs),)),
         pltpu.SemaphoreType.DMA(())],
        TYP * d * 2000, total * d * 4,
    )(meta)


def fwd_up(meta, xc, wts, layer, dy=None, n_p=1, deps=()):
    d, f = xc.shape[1], wts[0].shape[2]
    ch = 512
    steps = xc.shape[0] // TB
    fused = dy is not None
    n_w = len(wts)

    def body(meta, ins, outs, scr):
        x_ref = ins[0]
        parts = ins[1:1 + n_w]
        h_ref, a_ref = outs[:2]
        w, sem = scr[:2]
        t = pl.program_id(0)

        def activate(j, rs):
            sl = slice(j * ch, (j + 1) * ch)
            a_ref[rs, sl] = gelu_of(h_ref[rs, sl].astype(F32)).astype(BF)

        def share(i, rs):
            acc = scr[2]
            g = ins[1 + n_w][rs, :]
            col = pl.multiple_of((2 * i + 1 - meta[1]) * (f // 4), f // 4)
            part = lax.dot_general(a_ref[rs, pl.ds(col, f // 4)], g, TN, preferred_element_type=F32)
            acc[i] = part + jnp.where(t == 0, 0.0, acc[i])

        @pl.when(t == 0)
        def _():
            load_weight(meta, layer, parts, w, sem)

        def compute(rs):
            x = x_ref[rs, :]
            n = f // ch
            for j in range(n):
                sl = slice(j * ch, (j + 1) * ch)
                h_ref[rs, sl] = jnp.dot(x, w[:, sl], preferred_element_type=F32).astype(BF)
                if j:
                    activate(j - 1, rs)
                if fused and j == n // 2 + 1:
                    share(0, rs)
            activate(n - 1, rs)
            if fused:
                share(1, rs)

        live_tiles(meta, t, compute)

        if fused:
            gradient_out(t, meta[5] - 1, steps - 1, scr[2], outs[2:], scr[3])

    out = jax.ShapeDtypeStruct((xc.shape[0], f), BF)
    more_in, more_spec, more_out, more_ospec, more_scr = (), [], [], [], []
    if fused:
        shape = (2, f // 4, d)
        more_in, more_spec = (dy,), [tile(TB, d)]
        more_out = [jax.ShapeDtypeStruct((2, f // 4 // n_p, d), F32)] * n_p
        more_ospec = [ANY] * n_p
        more_scr = [pltpu.VMEM(shape, F32), pltpu.SemaphoreType.DMA((n_p,))]
    return call(
        body, (steps,), [tile(TB, d)] + [ANY] * n_w + more_spec, [tile(TB, f)] * 2 + more_ospec,
        [out, out] + more_out, (xc,) + wts + more_in, deps,
        [pltpu.VMEM((d, f), BF), pltpu.SemaphoreType.DMA((6,))] + more_scr,
        (3 if fused else 2) * TYP * d * f, TYP * (d + 2 * f) * 2,
    )(meta)


def fwd_down(meta, xc, a, wts, layer, deps=()):
    d, f = xc.shape[1], a.shape[1]
    ch = 512

    def body(meta, ins, outs, scr):
        x_ref, a_ref, *parts = ins
        (o_ref,) = outs
        w, sem = scr
        t = pl.program_id(0)

        @pl.when(t == 0)
        def _():
            load_weight(meta, layer, parts, w, sem)

        def compute(rs):
            for j in range(d // ch):
                sl = slice(j * ch, (j + 1) * ch)
                y = jnp.dot(a_ref[rs, :], w[:, sl], preferred_element_type=F32)
                o_ref[rs, sl] = (x_ref[rs, sl].astype(F32) + y).astype(BF)

        live_tiles(meta, t, compute)

    return call(
        body, (xc.shape[0] // TB,), [tile(TB, d), tile(TB, f)] + [ANY] * len(wts), [tile(TB, d)],
        [jax.ShapeDtypeStruct(xc.shape, BF)], (xc, a) + wts, deps,
        [pltpu.VMEM((f, d), BF), pltpu.SemaphoreType.DMA((6,))],
        2 * TYP * d * f, TYP * (2 * d + f) * 2,
    )(meta)


def fwd_layer(meta, xc, ups, downs, layer, deps=()):
    d, f = xc.shape[1], ups[0].shape[2]
    ch = 512
    n_up, n_w = len(ups), len(ups) + len(downs)

    def body(meta, ins, outs, scr):
        x_ref, *parts = ins
        h_ref, a_ref, o_ref = outs
        wu, wd, usem, dsem = scr
        t = pl.program_id(0)

        @pl.when(t == 0)
        def _():
            load_weight(meta, layer, parts[:n_up], wu, usem)
            load_weight(meta, layer, parts[n_up:], wd, dsem)

        def activate(j, rs):
            sl = slice(j * ch, (j + 1) * ch)
            a_ref[rs, sl] = gelu_of(h_ref[rs, sl].astype(F32)).astype(BF)

        def compute(rs):
            x = x_ref[rs, :]
            n = f // ch
            for j in range(n):
                sl = slice(j * ch, (j + 1) * ch)
                h_ref[rs, sl] = jnp.dot(x, wu[:, sl], preferred_element_type=F32).astype(BF)
                if j:
                    activate(j - 1, rs)
            activate(n - 1, rs)
            for j in range(d // ch):
                sl = slice(j * ch, (j + 1) * ch)
                y = jnp.dot(a_ref[rs, :], wd[:, sl], preferred_element_type=F32)
                o_ref[rs, sl] = (x_ref[rs, sl].astype(F32) + y).astype(BF)

        live_tiles(meta, t, compute)

    out = jax.ShapeDtypeStruct((xc.shape[0], f), BF)
    return call(
        body, (xc.shape[0] // TB,), [tile(TB, d)] + [ANY] * n_w, [tile(TB, f), tile(TB, f), tile(TB, d)],
        [out, out, jax.ShapeDtypeStruct(xc.shape, BF)], (xc,) + ups + downs, deps,
        [pltpu.VMEM((d, f), BF), pltpu.VMEM((f, d), BF),
         pltpu.SemaphoreType.DMA((6,)), pltpu.SemaphoreType.DMA((6,))],
        4 * TYP * d * f, TYP * (2 * d + 2 * f) * 2,
    )(meta)


def bwd_hidden(meta, dx, h, xl, wts, layer, part=0, n_parts=1, deps=()):
    d, f = dx.shape[1], h.shape[1] // n_parts
    ch = 512
    steps = dx.shape[0] // TB

    def body(meta, ins, outs, scr):
        dx_ref, h_ref, x0, x1, *parts = ins
        o_ref, share = outs
        w, acc, sem, osem = scr
        t = pl.program_id(0)

        @pl.when(t == 0)
        def _():
            load_weight(meta, layer, parts, w, sem, part)

        def add(j, rs):
            sl = slice(j * ch, (j + 1) * ch)
            for i, x_ref in enumerate((x0, x1)):
                part = lax.dot_general(x_ref[rs, :], o_ref[rs, sl], TN, preferred_element_type=F32)
                acc[i, :, sl] = part + jnp.where(t == 0, 0.0, acc[i, :, sl])

        def compute(rs):
            g = dx_ref[rs, :]
            n = f // ch
            for j in range(n):
                sl = slice(j * ch, (j + 1) * ch)
                da = lax.dot_general(g, w[sl, :], NT, preferred_element_type=F32)
                o_ref[rs, sl] = (da * gelu_grad_of(h_ref[rs, sl].astype(F32))).astype(BF)
                if j:
                    add(j - 1, rs)
            add(n - 1, rs)

        live_tiles(meta, t, compute)

        gradient_out(t, meta[5] - 1, steps - 1, acc, [share], osem)

    u = d // 4
    return call(
        body, (steps,),
        [tile(TB, d), tile(TB, f, lambda m: part), tile(TB, u, lambda m: 1 - m[1]), tile(TB, u, lambda m: 3 - m[1])]
        + [ANY] * len(wts),
        [tile(TB, f), ANY],
        [jax.ShapeDtypeStruct((h.shape[0], f), BF), jax.ShapeDtypeStruct((2, u, f), F32)], (dx, h, xl, xl) + wts, deps,
        [pltpu.VMEM((f, d), BF), pltpu.VMEM((2, u, f), F32), pltpu.SemaphoreType.DMA((6,)), pltpu.SemaphoreType.DMA((1,))],
        3 * TYP * d * f, TYP * (d + 2 * f) * 2,
    )(meta)


def bwd_input(meta, dx, dhs, a, wts, layer, deps=()):
    d, f = dx.shape[1], 2 * dhs[0].shape[1]
    ch = 256
    steps = dx.shape[0] // TB
    u = f // 4

    def body(meta, ins, outs, scr):
        dx_ref, dh0, dh1, a0, a1, *parts = ins
        o_ref, share = outs
        w, acc, sem, osem = scr
        t = pl.program_id(0)

        @pl.when(t == 0)
        def _():
            load_weight(meta, layer, parts, w, sem)

        def compute(rs):
            for j in range(d // ch):
                sl = slice(j * ch, (j + 1) * ch)
                y = lax.dot_general(dh0[rs, :], w[sl, :f // 2], NT, preferred_element_type=F32)
                y = y + lax.dot_general(dh1[rs, :], w[sl, f // 2:], NT, preferred_element_type=F32)
                o_ref[rs, sl] = (dx_ref[rs, sl].astype(F32) + y).astype(BF)
            for i, a_ref in enumerate((a0, a1)):
                for r in range(0, u, 256):
                    part = lax.dot_general(a_ref[rs, r:r + 256], o_ref[rs, :], TN, preferred_element_type=F32)
                    acc[i, r:r + 256, :] = part + jnp.where(t == 0, 0.0, acc[i, r:r + 256, :])

        live_tiles(meta, t, compute)

        gradient_out(t, meta[5] - 1, steps - 1, acc, [share], osem)

    return call(
        body, (steps,),
        [tile(TB, d), tile(TB, f // 2), tile(TB, f // 2), tile(TB, u, lambda m: 1 - m[1]), tile(TB, u, lambda m: 3 - m[1])]
        + [ANY] * len(wts),
        [tile(TB, d), ANY],
        [jax.ShapeDtypeStruct(dx.shape, BF), jax.ShapeDtypeStruct((2, u, d), F32)], (dx, *dhs, a, a) + wts, deps,
        [pltpu.VMEM((d, f), BF), pltpu.VMEM((2, u, d), F32), pltpu.SemaphoreType.DMA((6,)), pltpu.SemaphoreType.DMA((1,))],
        3 * TYP * d * f, TYP * (2 * d + f) * 2,
    )(meta)


def grad(meta, kind, which, v, g, p, n_p, share, moved, deps=()):
    d = g.shape[1] if kind == "d" else v.shape[1]
    f = v.shape[1] if kind == "d" else g.shape[1]
    rows, cols = (f // 4 // n_p, d) if kind == "d" else (d // 4, f // n_p)
    adds = (share,) if moved is None else (share, moved)
    n_add = len(adds)

    def body(meta, ins, outs, scr):
        v_hbm, g_hbm = ins[:2]
        vbuf, gbuf, acc, ebuf, vsem, gsem, esem, osem = scr
        x, c, nb = meta[0], meta[1], meta[5]
        xb = x if which == "K" else 1 - x
        shard = 2 * xb + c

        def copies(t, slot):
            row = pl.ds(pl.multiple_of(t * TB, TB), TB)
            col = (shard * n_p + p) * rows if kind == "d" else shard * rows
            v_src = v_hbm.at[row, pl.ds(pl.multiple_of(col, rows), rows)]
            g_src = g_hbm.at[row] if kind == "d" else g_hbm.at[row, pl.ds(p * cols, cols)]
            return [
                pltpu.make_async_copy(v_src, vbuf.at[slot], vsem.at[slot]),
                pltpu.make_async_copy(g_src, gbuf.at[slot], gsem.at[slot]),
            ]

        def fetch(t, slot):
            for cp in copies(t, slot):
                cp.start()

        for k in range(NBUF - 1):
            @pl.when(k < nb)
            def _(k=k):
                fetch(k, k)

        if share.shape[1:] == (rows, cols):
            src = ins[2].at[xb]
        elif kind == "d":
            src = ins[2].at[xb, pl.ds(p * rows, rows)]
        else:
            src = ins[2].at[xb, :, pl.ds(p * cols, cols)]
        adding = [pltpu.make_async_copy(src, ebuf.at[0], esem.at[0])]
        if moved is not None:
            adding.append(pltpu.make_async_copy(ins[3], ebuf.at[1], esem.at[1]))
        if kind == "d":
            tiles = [(pl.ds(r, 256), pl.ds(0, cols)) for r in range(0, rows, 256)]
        else:
            tiles = [(pl.ds(0, rows), pl.ds(k, 1024)) for k in range(0, cols, 1024)]

        def send(rs, cs):
            return pltpu.make_async_copy(acc.at[rs, cs], outs[0].at[rs, cs], osem)

        def step(t, final, tokens=TB):
            slot = lax.rem(t, NBUF)
            nxt = t + NBUF - 1

            @pl.when(nxt < nb)
            def _():
                fetch(nxt, lax.rem(nxt, NBUF))

            for cp in copies(t, slot):
                cp.wait()

            @pl.when(t == 0)
            def _():
                for cp in adding:
                    cp.start()

            if final:
                for cp in adding:
                    cp.wait()
            for n, (rs, cs) in enumerate(tiles):
                part = lax.dot_general(
                    vbuf[slot, :tokens, rs], gbuf[slot, :tokens, cs], TN, preferred_element_type=F32
                )
                part = part + jnp.where(t == 0, 0.0, acc[rs, cs])
                if final:
                    for k in range(n_add):
                        part = part + ebuf[k, rs, cs]
                acc[rs, cs] = part
                if final and n:
                    send(*tiles[n - 1]).start()
            if final:
                send(*tiles[-1]).start()

        def loop(t, carry):
            step(t, False)
            return carry

        lax.fori_loop(0, nb - 1, loop, 0)
        whole = meta[6] == nb
        for tokens, here in ((TB, whole), (TB // 2, jnp.logical_not(whole))):
            @pl.when(here)
            def _(tokens=tokens):
                step(nb - 1, True, tokens)

        for part in tiles:
            send(*part).wait()

    scratch = [
        pltpu.VMEM((NBUF, TB, rows), BF),
        pltpu.VMEM((NBUF, TB, cols), BF),
        pltpu.VMEM((rows, cols), F32),
        pltpu.VMEM((n_add, rows, cols), F32),
        pltpu.SemaphoreType.DMA((NBUF,)),
        pltpu.SemaphoreType.DMA((NBUF,)),
        pltpu.SemaphoreType.DMA((2,)),
        pltpu.SemaphoreType.DMA(()),
    ]
    return call(
        body, (1,), [ANY] * (2 + n_add), [ANY], [jax.ShapeDtypeStruct((rows, cols), F32)], (v, g) + adds, deps, scratch,
        TYP * d * f // 2 // n_p, TYP * (d + f) // n_p * 2,
    )(meta)


def finish(meta, buf, mine, theirs, shape, layer, row, col, deps=()):
    rows, cols = mine.shape
    br, bc = min(rows, 256), min(cols, 1024)

    def body(meta, ins, outs, scr):
        outs[0][0] = ins[0][...] + ins[1][...]

    args = (mine, theirs) if buf is None else (mine, theirs, buf)
    part = pl.BlockSpec((br, bc), lambda i, j, m: (i, j))
    return call(
        body, (rows // br, cols // bc), [part, part] + [ANY] * (len(args) - 2),
        [pl.BlockSpec((1, br, bc), lambda i, j, m: (layer, row // br + i, col // bc + j))],
        [jax.ShapeDtypeStruct(shape, F32)], args, deps, [], 0, rows * cols * 12,
        None if buf is None else {3: 0},
    )(meta)


PIECES = {("d", 3): 2, ("d", 0): 2, ("u", 0): 4, ("u", 3): 2, ("u", 2): 2, ("u", 1): 2}
ORDER = [
    ("S", "d", 3, 0), ("B1", 3, 1), ("S", "d", 3, 1), ("S", "u", 3, 1), ("B1", 3, 0), ("K", "d", 3, 1), ("dx", 3),
    ("S", "u", 3, 0), ("K", "d", 3, 0), ("K", "u", 3, 1), ("S", "d", 2, 0), ("B1", 2, 1), ("K", "u", 3, 0),
    ("B1", 2, 0), ("S", "u", 2, 1), ("S", "u", 2, 0), ("K", "d", 2, 0), ("dx", 2), ("K", "u", 2, 1),
    ("S", "d", 1, 0), ("B1", 1, 0), ("K", "u", 2, 0), ("B1", 1, 1), ("K", "d", 1, 0), ("S", "u", 1, 1),
    ("S", "u", 1, 0), ("dx", 1), ("K", "u", 1, 1), ("S", "d", 0, 1), ("S", "d", 0, 0), ("K", "u", 1, 0),
    ("B1", 0, 1), ("K", "d", 0, 1), ("B1", 0, 0), ("K", "d", 0, 0), ("S", "u", 0, 0), ("S", "u", 0, 3),
    ("S", "u", 0, 1), ("PUT", "u", 3, 1), ("PUT", "d", 3, 1), ("K", "u", 0, 0), ("PUT", "u", 2, 1),
    ("PUT", "d", 0, 1), ("PUT", "d", 2, 0), ("K", "u", 0, 3), ("S", "u", 0, 2), ("PUT", "u", 0, 0),
    ("PUT", "u", 1, 1), ("K", "u", 0, 1), ("PUT", "d", 0, 0), ("PUT", "d", 3, 0), ("PUT", "u", 1, 0),
    ("K", "u", 0, 2), ("PUT", "u", 0, 3), ("PUT", "u", 3, 0), ("PUT", "u", 2, 0), ("PUT", "u", 0, 1),
    ("PUT", "d", 1, 0), ("PUT", "u", 0, 2),
]


def pieces_of(kind, layer):
    return PIECES.get((kind, layer), 1)


def solution(mesh):
    tok_spec = P(None, ("model", "replica", "fsdp"), None)
    len_spec = P(None, ("model", "replica", "fsdp"))
    w_spec = P(None, ("model", "fsdp"), None)

    def device_grads(x_in, dy_out, lengths, w_up, w_down):
        n_micro, tok, d = x_in.shape
        n_layers, unit_d, f = w_up.shape
        unit_f = w_down.shape[1]
        fi = lax.axis_index("fsdp")
        yi = lax.axis_index("replica")

        def swap(v):
            return lax.ppermute(v, "fsdp", SWAP_CORE)

        def swap_y(v):
            return lax.ppermute(v, "replica", [(0, 1), (1, 0)])

        mats = [(w, l) for l in range(n_layers) for w in (w_up, w_down)]

        def half(w, l):
            n = w.shape[1] // 2
            return lax.dynamic_slice(w, (l, yi * n, 0), (1, n, w.shape[2]))[0]

        held = {id(w): lax.optimization_barrier(w) for w in (w_up, w_down)}
        far_x = []
        for i, (w, l) in enumerate(mats):
            src = w[l] if i == 0 else held[id(w)][l] if i in WHOLE else half(held[id(w)], l)
            far_x.append(lax.ppermute(src, "fsdp", SWAP_X))
        par = {}
        for w in (w_up, w_down):
            par[id(w)] = swap(w)
        parts = []
        for i, (w, l) in enumerate(mats):
            far = [far_x[i]]
            if i not in WHOLE:
                far.append(swap_y(far_x[i]))
            far.append(swap(far_x[i]))
            if i not in WHOLE:
                far.append(swap(far[1]))
            parts.append((w, par[id(w)], *far))
        ups, downs = parts[0::2], parts[1::2]

        def to_class(v, cls):
            step = CLASS_STEP[cls - 1]
            return lax.ppermute(v, ("replica", "fsdp"), [(i, i ^ step) for i in range(8)])

        lens = [lengths[:, 0]]
        for cls in (1, 2, 3):
            lens.append(to_class(lengths, cls)[:, 0])
        counts = [count_of(lens[cls], cls, tok)[k] for cls in range(4) for k in range(n_micro)]
        total = sum((n + 15) // 16 for n in counts)
        n_tok = total * 16
        nb = (n_tok + TB - 1) // TB
        n_full = (n_tok + TB // 2 - 1) // TB
        meta = jnp.stack([fi // 2, fi % 2, yi, n_tok, nb, nb, n_full, nb] + counts).astype(jnp.int32)

        def exchange(v, deps):
            v = v.reshape(n_micro, tok // BLK, BLK, d)
            *parts, done = split(v, deps=deps)
            gots = []
            for cls in (1, 2, 3):
                gots.append(to_class(parts[cls - 1], cls))
            return v, gots, done

        x_own, x_gots, tok_ = exchange(x_in, ())
        dy_own, dy_gots, tok_ = exchange(dy_out, (tok_,))
        xc, tok_ = pack(meta, x_own, x_gots, False, deps=(tok_,))
        dxs = {}

        top = n_layers - 1
        h, a, tok_ = fwd_up(meta, xc, ups[0], 0, deps=(tok_,))
        x, tok_ = fwd_down(meta, xc, a, downs[0], 0, deps=(tok_,))
        xs, hs, acts = [xc, x], [h], [a]
        for l in range(1, top):
            if l == 2:
                dxs[n_layers], tok_ = pack(meta, dy_own, dy_gots, True, deps=(tok_,))
            h, a, x, tok_ = fwd_layer(meta, xs[-1], ups[l], downs[l], l, deps=(tok_,))
            xs.append(x)
            hs.append(h)
            acts.append(a)
        h, a, *parts, tok_ = fwd_up(
            meta, xs[-1], ups[top], top, dy=dxs[n_layers], n_p=pieces_of("d", top), deps=(tok_,)
        )
        hs.append(h)
        acts.append(a)
        shares = {("d", top, p): swap(v) for p, v in enumerate(parts)}

        dhs, moved, sums = {}, {}, {}
        bufs = {"d": None, "u": None}
        shapes = {"d": (n_layers, unit_f, d), "u": (n_layers, unit_d, f)}
        for what, *key in ORDER:
            key = tuple(key)
            if what == "B1":
                l, part = key
                dhs[key], out, tok_ = bwd_hidden(
                    meta, dxs[l + 1], hs[l], xs[l], downs[l], l, part, 2, deps=(tok_,)
                )
            elif what == "dx":
                l = key[0]
                dh = (dhs[l, 0], dhs[l, 1])
                dxs[l], out, tok_ = bwd_input(meta, dxs[l + 1], dh, acts[l - 1], ups[l], l, deps=(tok_,))
            elif what == "PUT":
                kind, l, p = key
                row = p * unit_f // pieces_of(kind, l) if kind == "d" else 0
                col = 0 if kind == "d" else p * f // pieces_of(kind, l)
                bufs[kind], tok_ = finish(meta, bufs[kind], *sums[key], shapes[kind], l, row, col, deps=(tok_,))
            else:
                kind, l, p = key
                n_p = pieces_of(kind, l)
                if kind == "d":
                    v, g, at = acts[l], dxs[l + 1], (p, n_p)
                    share = shares.get(key, shares.get(key[:2]))
                else:
                    part, n_p = p * 2 // n_p, n_p // 2
                    v, g, at, share = xs[l], dhs[l, part], (p % n_p, n_p), shares[kind, l, part]
                out, tok_ = grad(meta, kind, what, v, g, *at, share, moved[key] if what == "K" else None, deps=(tok_,))
            if what == "B1":
                shares["u", *key] = swap(out)
            elif what == "dx":
                shares["d", l - 1] = swap(out)
            elif what == "S":
                moved[key] = lax.ppermute(out, "fsdp", SWAP_X)
            elif what == "K":
                sums[key] = (out, swap_y(out))

        return bufs["u"], bufs["d"]

    return jax.shard_map(
        device_grads, mesh=mesh, in_specs=(tok_spec, tok_spec, len_spec, w_spec, w_spec),
        out_specs=(w_spec, w_spec), check_vma=False,
    )
```

```python
import jax
import jax.numpy as jnp
from jax import lax
from jax.experimental import pallas as pl
from jax.experimental.pallas import tpu as pltpu
from jax.sharding import PartitionSpec as P


BF = jnp.bfloat16
F32 = jnp.float32
BLK = 32
TB = 512
NBUF = 3
K0 = 0.7978845608028654
K1 = 0.044715
TYP = 3584
SWAP_CORE = [(0, 1), (1, 0), (2, 3), (3, 2)]
SWAP_X = [(0, 2), (2, 0), (1, 3), (3, 1)]
WHOLE = (0, 3, 5, 6, 7)
CLASS_STEP = (1, 4, 5)
ANY = pl.BlockSpec(memory_space=pl.ANY)
NT = (((1,), (1,)), ((), ()))
TN = (((0,), (0,)), ((), ()))


def gelu_of(h):
    return h * (0.5 + 0.5 * jnp.tanh(h * (K0 + (K0 * K1) * (h * h))))


def gelu_grad_of(h):
    hh = h * h
    s = 0.5 + 0.5 * jnp.tanh(h * (K0 + (K0 * K1) * hh))
    return s + ((s * (1.0 - s)) * h) * ((2.0 * K0) + (6.0 * K0 * K1) * hh)


def load_weight(meta, layer, parts, w, sem, first=0):
    own, par, *far = parts
    x, c, y = meta[0], meta[1], meta[2]
    unit = own.shape[1]
    half = unit // 2
    o = 1 - x
    mine, other = (2 * o + c) * unit, (2 * o + 1 - c) * unit
    rows = [(own.at[layer], (2 * x + c) * unit, unit), (par.at[layer], (2 * x + 1 - c) * unit, unit)]
    if len(far) == 2:
        rows += [(far[0], mine, unit), (far[1], other, unit)]
    else:
        low, high = y * half, (1 - y) * half
        rows += [(far[0], mine + low, half), (far[1], mine + high, half)]
        rows += [(far[2], other + low, half), (far[3], other + high, half)]
    size = w.shape[0]

    def each(act):
        for k, (src, row, n) in enumerate(rows):
            if size == 4 * unit:
                at = pl.multiple_of(row, half)
                act(pltpu.make_async_copy(src, w.at[pl.ds(at, n)], sem.at[k]))
            else:
                @pl.when(row // size == first)
                def _(src=src, row=row, n=n, k=k):
                    at = pl.multiple_of(row - first * size, half)
                    act(pltpu.make_async_copy(src, w.at[pl.ds(at, n)], sem.at[k]))

    each(lambda cp: cp.start())
    each(lambda cp: cp.wait())


def tile(rows, cols, col=None):
    pick = col or (lambda m: 0)
    return pl.BlockSpec((rows, cols), lambda t, m: (jnp.minimum(t, m[5] - 1), pick(m)))


def call(body, grid, in_specs, out_specs, out_shape, args, deps, scratch, flops, nbytes, aliases=None):
    n_in, n_dep, n_out = len(args), len(deps), len(out_shape)

    def kern(meta, *refs):
        rest = refs[n_in + n_dep:]
        body(meta, refs[:n_in], rest[:n_out], rest[n_out + 1:])

    def run(meta):
        return pl.pallas_call(
            kern,
            grid_spec=pltpu.PrefetchScalarGridSpec(
                num_scalar_prefetch=1,
                grid=grid,
                in_specs=list(in_specs) + [ANY] * n_dep,
                out_specs=list(out_specs) + [ANY],
                scratch_shapes=scratch,
            ),
            out_shape=list(out_shape) + [jax.ShapeDtypeStruct((8, 128), F32)],
            input_output_aliases=aliases or {},
            cost_estimate=pl.CostEstimate(flops=flops, bytes_accessed=nbytes, transcendentals=0),
            compiler_params=pltpu.CompilerParams(
                dimension_semantics=("arbitrary",) * len(grid), vmem_limit_bytes=67043328
            ),
        )(meta, *args, *deps)

    return run


def live_tiles(meta, t, compute):
    @pl.when(t < meta[6])
    def _():
        compute(slice(0, TB))

    @pl.when((t >= meta[6]) & (t < meta[5]))
    def _():
        compute(slice(0, TB // 2))


def gradient_out(t, last_live, last, acc, dsts, sem):
    n = acc.shape[1] // len(dsts)
    copies = [
        pltpu.make_async_copy(acc.at[:, pl.ds(k * n, n)], dst, sem.at[k]) for k, dst in enumerate(dsts)
    ]

    @pl.when(t == last_live)
    def _():
        for cp in copies:
            cp.start()

    @pl.when(t == last)
    def _():
        for cp in copies:
            cp.wait()


def blocks_of(cls, n_blk):
    low = n_blk // 2
    first = [b for b in range(low) if b % 2 == cls]
    return first + [b for b in range(low, n_blk) if (b - low) % 4 == cls]


def count_of(length, cls, tok):
    low = jnp.minimum(length, tok // 2)
    high = length - low

    def share(n, ways):
        return (n // (ways * BLK)) * BLK + jnp.clip(n % (ways * BLK) - cls * BLK, 0, BLK)

    return (share(low, 2) if cls < 2 else 0) + share(high, 4)


def split(v, deps=()):
    n_micro, n_blk, blk, d = v.shape
    lists = [blocks_of(cls, n_blk) for cls in (1, 2, 3)]

    def body(meta, ins, outs, scr):
        bufs, isem, osem = scr[:3], scr[3], scr[4]
        takes = [
            [
                pltpu.make_async_copy(ins[0].at[k, b], buf.at[k, pl.ds(n * blk, blk)], isem.at[c])
                for k in range(n_micro) for n, b in enumerate(lists[c])
            ]
            for c, buf in enumerate(bufs)
        ]
        gives = [pltpu.make_async_copy(buf, o, osem.at[c]) for c, (buf, o) in enumerate(zip(bufs, outs))]
        order = (1, 2, 0)
        for c in order:
            for cp in takes[c]:
                cp.start()
        for c in order:
            for cp in takes[c]:
                cp.wait()
            gives[c].start()
        for cp in gives:
            cp.wait()

    shapes = [(n_micro, len(x) * blk, d) for x in lists]
    return call(
        body, (1,), [ANY], [ANY] * 3, [jax.ShapeDtypeStruct(s, BF) for s in shapes], (v,), deps,
        [pltpu.VMEM(s, BF) for s in shapes] + [pltpu.SemaphoreType.DMA((3,))] * 2,
        TYP * d * 1000, n_micro * n_blk * blk * d * 3,
    )(jnp.zeros((1,), jnp.int32))


def pack(meta, v, gots, masked, deps=()):
    n_micro, n_blk, blk, d = v.shape
    mine = blocks_of(0, n_blk)
    total = n_micro * n_blk * blk
    seqs = [(None, k) for k in range(n_micro)] + [(c, k) for c in range(len(gots)) for k in range(n_micro)]
    longest = len(mine) * blk

    def body(meta, ins, outs, scr):
        v_hbm, *got = ins
        (o_hbm,) = outs
        buf, zero, isem, osem = scr
        takes = []
        for s, (c, k) in enumerate(seqs):
            if c is None:
                takes.append([
                    pltpu.make_async_copy(v_hbm.at[k, b], buf.at[s, pl.ds(n * blk, blk)], isem.at[s])
                    for n, b in enumerate(mine)
                ])
            else:
                n = gots[c].shape[1]
                takes.append([pltpu.make_async_copy(got[c].at[k], buf.at[s, pl.ds(0, n)], isem.at[s])])
        for copies in takes:
            for cp in copies:
                cp.start()
        zero[...] = jnp.zeros_like(zero)

        def pieces(src, off, n, largest):
            at, out = jnp.int32(0), []
            size = largest
            while size >= 16:
                on = (n // size) % 2 == 1
                here = pl.ds(pl.multiple_of(at, 16), size) if src is not zero else pl.ds(0, size)
                there = pl.ds(pl.multiple_of(off + at, 16), size)
                out.append((on, pltpu.make_async_copy(src.at[here], o_hbm.at[there], osem)))
                at = at + jnp.where(on, size, 0)
                size //= 2
            return out

        gives, off = [], jnp.int32(0)
        for s in range(len(seqs)):
            n = meta[8 + s]
            for cp in takes[s]:
                cp.wait()
            if masked:
                base = n // 16 * 16

                @pl.when(n > base)
                def _(s=s, n=n, base=base):
                    row = pl.ds(pl.multiple_of(base, 16), 16)
                    at = lax.broadcasted_iota(jnp.int32, (16, d), 0) + base
                    buf[s, row, :] = jnp.where(at < n, buf[s, row, :].astype(F32), 0.0).astype(BF)

            n = (n + 15) // 16 * 16
            for on, cp in pieces(buf.at[s], off, n, 512):
                gives.append((on, cp))
                pl.when(on)(cp.start)
            off = off + n
        for on, cp in pieces(zero, off, meta[5] * TB - off, 256):
            gives.append((on, cp))
            pl.when(on)(cp.start)
        for on, cp in gives:
            pl.when(on)(cp.wait)

    return call(
        body, (1,), [ANY] * (1 + len(gots)), [ANY], [jax.ShapeDtypeStruct((total, d), BF)], (v,) + tuple(gots), deps,
        [pltpu.VMEM((len(seqs), longest, d), BF), pltpu.VMEM((TB // 2, d), BF), pltpu.SemaphoreType.DMA((len(seqs),)),
         pltpu.SemaphoreType.DMA(())],
        TYP * d * 2000, total * d * 4,
    )(meta)


def fwd_up(meta, xc, wts, layer, dy=None, n_p=1, deps=()):
    d, f = xc.shape[1], wts[0].shape[2]
    ch = 512
    steps = xc.shape[0] // TB
    fused = dy is not None
    n_w = len(wts)

    def body(meta, ins, outs, scr):
        x_ref = ins[0]
        parts = ins[1:1 + n_w]
        h_ref, a_ref = outs[:2]
        w, sem = scr[:2]
        t = pl.program_id(0)

        def activate(j, rs):
            sl = slice(j * ch, (j + 1) * ch)
            a_ref[rs, sl] = gelu_of(h_ref[rs, sl].astype(F32)).astype(BF)

        def share(i, rs):
            acc = scr[2]
            g = ins[1 + n_w][rs, :]
            col = pl.multiple_of((2 * i + 1 - meta[1]) * (f // 4), f // 4)
            part = lax.dot_general(a_ref[rs, pl.ds(col, f // 4)], g, TN, preferred_element_type=F32)
            acc[i] = part + jnp.where(t == 0, 0.0, acc[i])

        @pl.when(t == 0)
        def _():
            load_weight(meta, layer, parts, w, sem)

        def compute(rs):
            x = x_ref[rs, :]
            n = f // ch
            for j in range(n):
                sl = slice(j * ch, (j + 1) * ch)
                h_ref[rs, sl] = jnp.dot(x, w[:, sl], preferred_element_type=F32).astype(BF)
                if j:
                    activate(j - 1, rs)
                if fused and j == n // 2 + 1:
                    share(0, rs)
            activate(n - 1, rs)
            if fused:
                share(1, rs)

        live_tiles(meta, t, compute)

        if fused:
            gradient_out(t, meta[5] - 1, steps - 1, scr[2], outs[2:], scr[3])

    out = jax.ShapeDtypeStruct((xc.shape[0], f), BF)
    more_in, more_spec, more_out, more_ospec, more_scr = (), [], [], [], []
    if fused:
        shape = (2, f // 4, d)
        more_in, more_spec = (dy,), [tile(TB, d)]
        more_out = [jax.ShapeDtypeStruct((2, f // 4 // n_p, d), F32)] * n_p
        more_ospec = [ANY] * n_p
        more_scr = [pltpu.VMEM(shape, F32), pltpu.SemaphoreType.DMA((n_p,))]
    return call(
        body, (steps,), [tile(TB, d)] + [ANY] * n_w + more_spec, [tile(TB, f)] * 2 + more_ospec,
        [out, out] + more_out, (xc,) + wts + more_in, deps,
        [pltpu.VMEM((d, f), BF), pltpu.SemaphoreType.DMA((6,))] + more_scr,
        (3 if fused else 2) * TYP * d * f, TYP * (d + 2 * f) * 2,
    )(meta)


def fwd_down(meta, xc, a, wts, layer, deps=()):
    d, f = xc.shape[1], a.shape[1]
    ch = 512

    def body(meta, ins, outs, scr):
        x_ref, a_ref, *parts = ins
        (o_ref,) = outs
        w, sem = scr
        t = pl.program_id(0)

        @pl.when(t == 0)
        def _():
            load_weight(meta, layer, parts, w, sem)

        def compute(rs):
            for j in range(d // ch):
                sl = slice(j * ch, (j + 1) * ch)
                y = jnp.dot(a_ref[rs, :], w[:, sl], preferred_element_type=F32)
                o_ref[rs, sl] = (x_ref[rs, sl].astype(F32) + y).astype(BF)

        live_tiles(meta, t, compute)

    return call(
        body, (xc.shape[0] // TB,), [tile(TB, d), tile(TB, f)] + [ANY] * len(wts), [tile(TB, d)],
        [jax.ShapeDtypeStruct(xc.shape, BF)], (xc, a) + wts, deps,
        [pltpu.VMEM((f, d), BF), pltpu.SemaphoreType.DMA((6,))],
        2 * TYP * d * f, TYP * (2 * d + f) * 2,
    )(meta)


def fwd_layer(meta, xc, ups, downs, layer, deps=()):
    d, f = xc.shape[1], ups[0].shape[2]
    ch = 512
    n_up, n_w = len(ups), len(ups) + len(downs)

    def body(meta, ins, outs, scr):
        x_ref, *parts = ins
        h_ref, a_ref, o_ref = outs
        wu, wd, usem, dsem = scr
        t = pl.program_id(0)

        @pl.when(t == 0)
        def _():
            load_weight(meta, layer, parts[:n_up], wu, usem)
            load_weight(meta, layer, parts[n_up:], wd, dsem)

        def activate(j, rs):
            sl = slice(j * ch, (j + 1) * ch)
            a_ref[rs, sl] = gelu_of(h_ref[rs, sl].astype(F32)).astype(BF)

        def compute(rs):
            x = x_ref[rs, :]
            n = f // ch
            for j in range(n):
                sl = slice(j * ch, (j + 1) * ch)
                h_ref[rs, sl] = jnp.dot(x, wu[:, sl], preferred_element_type=F32).astype(BF)
                if j:
                    activate(j - 1, rs)
            activate(n - 1, rs)
            for j in range(d // ch):
                sl = slice(j * ch, (j + 1) * ch)
                y = jnp.dot(a_ref[rs, :], wd[:, sl], preferred_element_type=F32)
                o_ref[rs, sl] = (x_ref[rs, sl].astype(F32) + y).astype(BF)

        live_tiles(meta, t, compute)

    out = jax.ShapeDtypeStruct((xc.shape[0], f), BF)
    return call(
        body, (xc.shape[0] // TB,), [tile(TB, d)] + [ANY] * n_w, [tile(TB, f), tile(TB, f), tile(TB, d)],
        [out, out, jax.ShapeDtypeStruct(xc.shape, BF)], (xc,) + ups + downs, deps,
        [pltpu.VMEM((d, f), BF), pltpu.VMEM((f, d), BF),
         pltpu.SemaphoreType.DMA((6,)), pltpu.SemaphoreType.DMA((6,))],
        4 * TYP * d * f, TYP * (2 * d + 2 * f) * 2,
    )(meta)


def bwd_hidden(meta, dx, h, xl, wts, layer, part=0, n_parts=1, deps=()):
    d, f = dx.shape[1], h.shape[1] // n_parts
    ch = 512
    steps = dx.shape[0] // TB

    def body(meta, ins, outs, scr):
        dx_ref, h_ref, x0, x1, *parts = ins
        o_ref, share = outs
        w, acc, sem, osem = scr
        t = pl.program_id(0)

        @pl.when(t == 0)
        def _():
            load_weight(meta, layer, parts, w, sem, part)

        def add(j, rs):
            sl = slice(j * ch, (j + 1) * ch)
            for i, x_ref in enumerate((x0, x1)):
                part = lax.dot_general(x_ref[rs, :], o_ref[rs, sl], TN, preferred_element_type=F32)
                acc[i, :, sl] = part + jnp.where(t == 0, 0.0, acc[i, :, sl])

        def compute(rs):
            g = dx_ref[rs, :]
            n = f // ch
            for j in range(n):
                sl = slice(j * ch, (j + 1) * ch)
                da = lax.dot_general(g, w[sl, :], NT, preferred_element_type=F32)
                o_ref[rs, sl] = (da * gelu_grad_of(h_ref[rs, sl].astype(F32))).astype(BF)
                if j:
                    add(j - 1, rs)
            add(n - 1, rs)

        live_tiles(meta, t, compute)

        gradient_out(t, meta[5] - 1, steps - 1, acc, [share], osem)

    u = d // 4
    return call(
        body, (steps,),
        [tile(TB, d), tile(TB, f, lambda m: part), tile(TB, u, lambda m: 1 - m[1]), tile(TB, u, lambda m: 3 - m[1])]
        + [ANY] * len(wts),
        [tile(TB, f), ANY],
        [jax.ShapeDtypeStruct((h.shape[0], f), BF), jax.ShapeDtypeStruct((2, u, f), F32)], (dx, h, xl, xl) + wts, deps,
        [pltpu.VMEM((f, d), BF), pltpu.VMEM((2, u, f), F32), pltpu.SemaphoreType.DMA((6,)), pltpu.SemaphoreType.DMA((1,))],
        3 * TYP * d * f, TYP * (d + 2 * f) * 2,
    )(meta)


def bwd_input(meta, dx, dhs, a, wts, layer, deps=()):
    d, f = dx.shape[1], 2 * dhs[0].shape[1]
    ch = 256
    steps = dx.shape[0] // TB
    u = f // 4

    def body(meta, ins, outs, scr):
        dx_ref, dh0, dh1, a0, a1, *parts = ins
        o_ref, share = outs
        w, acc, sem, osem = scr
        t = pl.program_id(0)

        @pl.when(t == 0)
        def _():
            load_weight(meta, layer, parts, w, sem)

        def compute(rs):
            for j in range(d // ch):
                sl = slice(j * ch, (j + 1) * ch)
                y = lax.dot_general(dh0[rs, :], w[sl, :f // 2], NT, preferred_element_type=F32)
                y = y + lax.dot_general(dh1[rs, :], w[sl, f // 2:], NT, preferred_element_type=F32)
                o_ref[rs, sl] = (dx_ref[rs, sl].astype(F32) + y).astype(BF)
            for i, a_ref in enumerate((a0, a1)):
                for r in range(0, u, 256):
                    part = lax.dot_general(a_ref[rs, r:r + 256], o_ref[rs, :], TN, preferred_element_type=F32)
                    acc[i, r:r + 256, :] = part + jnp.where(t == 0, 0.0, acc[i, r:r + 256, :])

        live_tiles(meta, t, compute)

        gradient_out(t, meta[5] - 1, steps - 1, acc, [share], osem)

    return call(
        body, (steps,),
        [tile(TB, d), tile(TB, f // 2), tile(TB, f // 2), tile(TB, u, lambda m: 1 - m[1]), tile(TB, u, lambda m: 3 - m[1])]
        + [ANY] * len(wts),
        [tile(TB, d), ANY],
        [jax.ShapeDtypeStruct(dx.shape, BF), jax.ShapeDtypeStruct((2, u, d), F32)], (dx, *dhs, a, a) + wts, deps,
        [pltpu.VMEM((d, f), BF), pltpu.VMEM((2, u, d), F32), pltpu.SemaphoreType.DMA((6,)), pltpu.SemaphoreType.DMA((1,))],
        3 * TYP * d * f, TYP * (2 * d + f) * 2,
    )(meta)


def grad(meta, kind, which, v, g, p, n_p, share, moved, deps=()):
    d = g.shape[1] if kind == "d" else v.shape[1]
    f = v.shape[1] if kind == "d" else g.shape[1]
    rows, cols = (f // 4 // n_p, d) if kind == "d" else (d // 4, f // n_p)
    adds = (share,) if moved is None else (share, moved)
    n_add = len(adds)

    def body(meta, ins, outs, scr):
        v_hbm, g_hbm = ins[:2]
        vbuf, gbuf, acc, ebuf, vsem, gsem, esem, osem = scr
        x, c, nb = meta[0], meta[1], meta[5]
        xb = x if which == "K" else 1 - x
        shard = 2 * xb + c

        def copies(t, slot):
            row = pl.ds(pl.multiple_of(t * TB, TB), TB)
            col = (shard * n_p + p) * rows if kind == "d" else shard * rows
            v_src = v_hbm.at[row, pl.ds(pl.multiple_of(col, rows), rows)]
            g_src = g_hbm.at[row] if kind == "d" else g_hbm.at[row, pl.ds(p * cols, cols)]
            return [
                pltpu.make_async_copy(v_src, vbuf.at[slot], vsem.at[slot]),
                pltpu.make_async_copy(g_src, gbuf.at[slot], gsem.at[slot]),
            ]

        def fetch(t, slot):
            for cp in copies(t, slot):
                cp.start()

        for k in range(NBUF - 1):
            @pl.when(k < nb)
            def _(k=k):
                fetch(k, k)

        if share.shape[1:] == (rows, cols):
            src = ins[2].at[xb]
        elif kind == "d":
            src = ins[2].at[xb, pl.ds(p * rows, rows)]
        else:
            src = ins[2].at[xb, :, pl.ds(p * cols, cols)]
        adding = [pltpu.make_async_copy(src, ebuf.at[0], esem.at[0])]
        if moved is not None:
            adding.append(pltpu.make_async_copy(ins[3], ebuf.at[1], esem.at[1]))
        if kind == "d":
            tiles = [(pl.ds(r, 256), pl.ds(0, cols)) for r in range(0, rows, 256)]
        else:
            tiles = [(pl.ds(0, rows), pl.ds(k, 1024)) for k in range(0, cols, 1024)]

        def send(rs, cs):
            return pltpu.make_async_copy(acc.at[rs, cs], outs[0].at[rs, cs], osem)

        def step(t, final, tokens=TB):
            slot = lax.rem(t, NBUF)
            nxt = t + NBUF - 1

            @pl.when(nxt < nb)
            def _():
                fetch(nxt, lax.rem(nxt, NBUF))

            for cp in copies(t, slot):
                cp.wait()

            @pl.when(t == 0)
            def _():
                for cp in adding:
                    cp.start()

            if final:
                for cp in adding:
                    cp.wait()
            for n, (rs, cs) in enumerate(tiles):
                part = lax.dot_general(
                    vbuf[slot, :tokens, rs], gbuf[slot, :tokens, cs], TN, preferred_element_type=F32
                )
                part = part + jnp.where(t == 0, 0.0, acc[rs, cs])
                if final:
                    for k in range(n_add):
                        part = part + ebuf[k, rs, cs]
                acc[rs, cs] = part
                if final and n:
                    send(*tiles[n - 1]).start()
            if final:
                send(*tiles[-1]).start()

        def loop(t, carry):
            step(t, False)
            return carry

        lax.fori_loop(0, nb - 1, loop, 0)
        whole = meta[6] == nb
        for tokens, here in ((TB, whole), (TB // 2, jnp.logical_not(whole))):
            @pl.when(here)
            def _(tokens=tokens):
                step(nb - 1, True, tokens)

        for part in tiles:
            send(*part).wait()

    scratch = [
        pltpu.VMEM((NBUF, TB, rows), BF),
        pltpu.VMEM((NBUF, TB, cols), BF),
        pltpu.VMEM((rows, cols), F32),
        pltpu.VMEM((n_add, rows, cols), F32),
        pltpu.SemaphoreType.DMA((NBUF,)),
        pltpu.SemaphoreType.DMA((NBUF,)),
        pltpu.SemaphoreType.DMA((2,)),
        pltpu.SemaphoreType.DMA(()),
    ]
    return call(
        body, (1,), [ANY] * (2 + n_add), [ANY], [jax.ShapeDtypeStruct((rows, cols), F32)], (v, g) + adds, deps, scratch,
        TYP * d * f // 2 // n_p, TYP * (d + f) // n_p * 2,
    )(meta)


def finish(meta, buf, mine, theirs, shape, layer, row, col, deps=()):
    rows, cols = mine.shape
    br, bc = min(rows, 256), min(cols, 1024)

    def body(meta, ins, outs, scr):
        outs[0][0] = ins[0][...] + ins[1][...]

    args = (mine, theirs) if buf is None else (mine, theirs, buf)
    part = pl.BlockSpec((br, bc), lambda i, j, m: (i, j))
    return call(
        body, (rows // br, cols // bc), [part, part] + [ANY] * (len(args) - 2),
        [pl.BlockSpec((1, br, bc), lambda i, j, m: (layer, row // br + i, col // bc + j))],
        [jax.ShapeDtypeStruct(shape, F32)], args, deps, [], 0, rows * cols * 12,
        None if buf is None else {3: 0},
    )(meta)


PIECES = {("d", 3): 2, ("d", 0): 2, ("u", 0): 4, ("u", 3): 2, ("u", 2): 2, ("u", 1): 2}
ORDER = [
    ("S", "d", 3, 0), ("B1", 3, 0), ("S", "d", 3, 1), ("B1", 3, 1), ("S", "u", 3, 0), ("S", "u", 3, 1),
    ("K", "d", 3, 1), ("dx", 3), ("K", "d", 3, 0), ("K", "u", 3, 0), ("S", "d", 2, 0), ("K", "u", 3, 1),
    ("B1", 2, 1), ("B1", 2, 0), ("S", "u", 2, 1), ("K", "d", 2, 0), ("S", "u", 2, 0), ("dx", 2), ("K", "u", 2, 1),
    ("S", "d", 1, 0), ("B1", 1, 1), ("K", "u", 2, 0), ("B1", 1, 0), ("K", "d", 1, 0), ("S", "u", 1, 1),
    ("S", "u", 1, 0), ("dx", 1), ("PUT", "u", 2, 1), ("K", "u", 1, 1), ("S", "d", 0, 0), ("S", "d", 0, 1),
    ("K", "u", 1, 0), ("B1", 0, 1), ("K", "d", 0, 0), ("B1", 0, 0), ("K", "d", 0, 1), ("S", "u", 0, 3),
    ("PUT", "u", 3, 1), ("S", "u", 0, 0), ("PUT", "u", 2, 0), ("PUT", "d", 1, 0), ("S", "u", 0, 2),
    ("K", "u", 0, 3), ("S", "u", 0, 1), ("PUT", "u", 3, 0), ("K", "u", 0, 0), ("PUT", "u", 1, 1),
    ("PUT", "u", 1, 0), ("PUT", "d", 0, 1), ("PUT", "d", 2, 0), ("K", "u", 0, 2), ("PUT", "d", 3, 0),
    ("PUT", "d", 3, 1), ("K", "u", 0, 1), ("PUT", "u", 0, 3), ("PUT", "u", 0, 2), ("PUT", "u", 0, 0),
    ("PUT", "d", 0, 0), ("PUT", "u", 0, 1),
]


def pieces_of(kind, layer):
    return PIECES.get((kind, layer), 1)


def solution(mesh):
    tok_spec = P(None, ("model", "replica", "fsdp"), None)
    len_spec = P(None, ("model", "replica", "fsdp"))
    w_spec = P(None, ("model", "fsdp"), None)

    def device_grads(x_in, dy_out, lengths, w_up, w_down):
        n_micro, tok, d = x_in.shape
        n_layers, unit_d, f = w_up.shape
        unit_f = w_down.shape[1]
        fi = lax.axis_index("fsdp")
        yi = lax.axis_index("replica")

        def swap(v):
            return lax.ppermute(v, "fsdp", SWAP_CORE)

        def swap_y(v):
            return lax.ppermute(v, "replica", [(0, 1), (1, 0)])

        mats = [(w, l) for l in range(n_layers) for w in (w_up, w_down)]

        def half(w, l):
            n = w.shape[1] // 2
            return lax.dynamic_slice(w, (l, yi * n, 0), (1, n, w.shape[2]))[0]

        held = {id(w): lax.optimization_barrier(w) for w in (w_up, w_down)}
        far_x = []
        for i, (w, l) in enumerate(mats):
            src = w[l] if i == 0 else held[id(w)][l] if i in WHOLE else half(held[id(w)], l)
            far_x.append(lax.ppermute(src, "fsdp", SWAP_X))
        par = {}
        for w in (w_up, w_down):
            par[id(w)] = swap(w)
        parts = []
        for i, (w, l) in enumerate(mats):
            far = [far_x[i]]
            if i not in WHOLE:
                far.append(swap_y(far_x[i]))
            far.append(swap(far_x[i]))
            if i not in WHOLE:
                far.append(swap(far[1]))
            parts.append((w, par[id(w)], *far))
        ups, downs = parts[0::2], parts[1::2]

        def to_class(v, cls):
            step = CLASS_STEP[cls - 1]
            return lax.ppermute(v, ("replica", "fsdp"), [(i, i ^ step) for i in range(8)])

        lens = [lengths[:, 0]]
        for cls in (1, 2, 3):
            lens.append(to_class(lengths, cls)[:, 0])
        counts = [count_of(lens[cls], cls, tok)[k] for cls in range(4) for k in range(n_micro)]
        total = sum((n + 15) // 16 for n in counts)
        n_tok = total * 16
        nb = (n_tok + TB - 1) // TB
        n_full = (n_tok + TB // 2 - 1) // TB
        meta = jnp.stack([fi // 2, fi % 2, yi, n_tok, nb, nb, n_full, nb] + counts).astype(jnp.int32)

        def exchange(v, deps):
            v = v.reshape(n_micro, tok // BLK, BLK, d)
            *parts, done = split(v, deps=deps)
            gots = []
            for cls in (1, 2, 3):
                gots.append(to_class(parts[cls - 1], cls))
            return v, gots, done

        x_own, x_gots, tok_ = exchange(x_in, ())
        dy_own, dy_gots, tok_ = exchange(dy_out, (tok_,))
        xc, tok_ = pack(meta, x_own, x_gots, False, deps=(tok_,))
        dxs = {}

        top = n_layers - 1
        h, a, tok_ = fwd_up(meta, xc, ups[0], 0, deps=(tok_,))
        x, tok_ = fwd_down(meta, xc, a, downs[0], 0, deps=(tok_,))
        xs, hs, acts = [xc, x], [h], [a]
        for l in range(1, top):
            if l == 2:
                dxs[n_layers], tok_ = pack(meta, dy_own, dy_gots, True, deps=(tok_,))
            h, a, x, tok_ = fwd_layer(meta, xs[-1], ups[l], downs[l], l, deps=(tok_,))
            xs.append(x)
            hs.append(h)
            acts.append(a)
        h, a, *parts, tok_ = fwd_up(
            meta, xs[-1], ups[top], top, dy=dxs[n_layers], n_p=pieces_of("d", top), deps=(tok_,)
        )
        hs.append(h)
        acts.append(a)
        shares = {("d", top, p): swap(v) for p, v in enumerate(parts)}

        dhs, moved, sums = {}, {}, {}
        bufs = {"d": None, "u": None}
        shapes = {"d": (n_layers, unit_f, d), "u": (n_layers, unit_d, f)}
        for what, *key in ORDER:
            key = tuple(key)
            if what == "B1":
                l, part = key
                dhs[key], out, tok_ = bwd_hidden(
                    meta, dxs[l + 1], hs[l], xs[l], downs[l], l, part, 2, deps=(tok_,)
                )
            elif what == "dx":
                l = key[0]
                dh = (dhs[l, 0], dhs[l, 1])
                dxs[l], out, tok_ = bwd_input(meta, dxs[l + 1], dh, acts[l - 1], ups[l], l, deps=(tok_,))
            elif what == "PUT":
                kind, l, p = key
                row = p * unit_f // pieces_of(kind, l) if kind == "d" else 0
                col = 0 if kind == "d" else p * f // pieces_of(kind, l)
                bufs[kind], tok_ = finish(meta, bufs[kind], *sums[key], shapes[kind], l, row, col, deps=(tok_,))
            else:
                kind, l, p = key
                n_p = pieces_of(kind, l)
                if kind == "d":
                    v, g, at = acts[l], dxs[l + 1], (p, n_p)
                    share = shares.get(key, shares.get(key[:2]))
                else:
                    part, n_p = p * 2 // n_p, n_p // 2
                    v, g, at, share = xs[l], dhs[l, part], (p % n_p, n_p), shares[kind, l, part]
                out, tok_ = grad(meta, kind, what, v, g, *at, share, moved[key] if what == "K" else None, deps=(tok_,))
            if what == "B1":
                shares["u", *key] = swap(out)
            elif what == "dx":
                shares["d", l - 1] = swap(out)
            elif what == "S":
                moved[key] = lax.ppermute(out, "fsdp", SWAP_X)
            elif what == "K":
                sums[key] = (out, swap_y(out))

        return bufs["u"], bufs["d"]

    return jax.shard_map(
        device_grads, mesh=mesh, in_specs=(tok_spec, tok_spec, len_spec, w_spec, w_spec),
        out_specs=(w_spec, w_spec), check_vma=False,
    )
```
